32 devices in a mesh: batch: 16 (over z, y, core), rows: 2 (over x).
Axes of the slice: x: 2, y: 2, z: 4, core: 2. Of those that a mesh axis runs over, the one named last changes fastest.
Arguments:
- block_input: bfloat16 [16, 16, 64, 384], P('batch', 'rows'), may hold values from -6 to 6
- output_grad: bfloat16 [16, 16, 64, 768], P('batch', 'rows'), may hold values from -6 to 6
- conv_weight: float32 [384, 1152], P(None, 'batch'), may hold values from -12 to 12
- conv_gain: float32 [384], replicated, may hold values from 0.1 to 1.9
- conv_momentum: float32 [384, 1152], P(None, 'batch'), may hold values from -0.6 to 0.6
- proj_weight: float32 [768, 384], P(None, 'batch'), may hold values from -12 to 12
- proj_gain: float32 [768], replicated, may hold values from 0.1 to 1.9
- proj_momentum: float32 [768, 384], P(None, 'batch'), may hold values from -0.6 to 0.6
Outputs:
- input_grad: bfloat16 [16, 16, 64, 384], P('batch', 'rows')
- new_conv_weight: float32 [384, 1152], P(None, 'batch')
- new_conv_momentum: float32 [384, 1152], P(None, 'batch')
- new_proj_weight: float32 [768, 384], P(None, 'batch')
- new_proj_momentum: float32 [768, 384], P(None, 'batch')
The draws below stay inside these ranges and needn't reach their ends.
All inputs are finite; a program needn't handle non-finite values.
Results may differ from the reference program's by a relative error of at most 0.0031.
The reference program's roundings to bfloat16 on the way (of `standard`, `activated`, `hidden` and `pre_grad`) count: a program that leaves them out, or rounds other values in their place, can miss the bound.
Values may be sent and summed in bfloat16 or wider, within the bound.
A program may use at most 64 MiB of HBM per device.

```python
import math
import jax
import jax.numpy as jnp
from jax import lax

CH = 384
GW = 128
OUT = 768
COLS = 64
IMAGES = 16
MAP_ROWS = 16


def scaled_rows(key, row_count, col_count):
    key_scale, key_body = jax.random.split(key)
    log_scale = jax.random.uniform(key_scale, (row_count, 1), jnp.float32, math.log(0.3), math.log(3.0))
    values = jax.random.truncated_normal(key_body, -4.0, 4.0, (row_count, col_count), jnp.float32)
    return jnp.exp(log_scale) * values


def draw_conv_weight(key, part):
    return scaled_rows(jax.random.fold_in(key, 11), CH, 9 * GW)


def draw_proj_weight(key, part):
    return scaled_rows(jax.random.fold_in(key, 23), OUT, CH)


def levels(stream_key, shape, pieces, low, largest):
    def one(axis_at, parts):
        heights = jax.random.uniform(jax.random.fold_in(jax.random.fold_in(stream_key, 6), axis_at), (parts,), jnp.float32, low / len(pieces), largest / len(pieces))
        return jnp.repeat(jnp.exp(heights), shape[axis_at] // parts).reshape((-1,) + (1,) * (len(shape) - axis_at - 1))

    level = one(*pieces[0])
    for cut in pieces[1:]:
        level = level * one(*cut)
    return level


def normal_values(stream_key, dims, width, most, cuts=(), dtype=jnp.bfloat16):
    factor_of = levels(stream_key, dims, cuts, -0.22, 0.18) if cuts else 1.0
    values = jax.random.normal(stream_key, dims, jnp.float32) * width * factor_of
    return jnp.minimum(jnp.maximum(values, -most), most).astype(dtype)


def setup_inputs(seed: int = 0) -> dict:
    arg_keys = jax.random.split(jax.random.key(seed), 9)
    return {
        "block_input": normal_values(arg_keys[0], (IMAGES, MAP_ROWS, COLS, CH), 1.0, 6.0, ((0, 16), (1, 2))),
        "output_grad": normal_values(arg_keys[1], (IMAGES, MAP_ROWS, COLS, OUT), 1.0, 6.0, ((0, 16), (1, 2))),
        "conv_weight": draw_conv_weight(jax.random.fold_in(arg_keys[8], 71), 0),
        "conv_gain": jnp.clip(1.0 + 0.18 * jax.random.normal(arg_keys[3], (CH,), jnp.float32), 0.1, 1.9),
        "conv_momentum": normal_values(arg_keys[4], (CH, 9 * GW), 0.1, 0.6, ((1, 16),), jnp.float32),
        "proj_weight": draw_proj_weight(jax.random.fold_in(arg_keys[8], 71), 0),
        "proj_gain": jnp.clip(1.0 + 0.18 * jax.random.normal(arg_keys[6], (OUT,), jnp.float32), 0.1, 1.9),
        "proj_momentum": normal_values(arg_keys[7], (OUT, CH), 0.1, 0.6, ((1, 16),), jnp.float32),
    }


ws_eps = 0.0001
clip_ratio = 0.05
momentum_rate = 0.9
learn_rate = 1.6
norm_eps = 1e-06

def gelu_slope(values):
    return jax.jvp(jax.nn.gelu, (values,), (jnp.ones_like(values),))[1]

def standardize(weight, gain_row):
    center = lax.optimization_barrier(jnp.mean(weight, axis=1, keepdims=True))
    centered = weight - center
    spread = lax.optimization_barrier(jnp.sum(centered * centered, axis=1))
    factor = lax.rsqrt(spread + ws_eps)
    standard = ((gain_row * factor)[:, None] * centered).astype(jnp.bfloat16)
    return (standard, centered, factor)

def apply_update(weight, momentum, raw_grad, weight_sq, grad_sq):
    clip_scale = jnp.minimum(1.0, clip_ratio * jnp.sqrt(weight_sq) * lax.rsqrt(grad_sq + norm_eps))
    clipped = raw_grad * clip_scale[:, None]
    new_momentum = momentum_rate * momentum + clipped
    return (weight - learn_rate * (clipped + momentum_rate * new_momentum), new_momentum)

def update(weight, gain_row, momentum, centered, factor, grad_std):
    fan_in = weight.shape[1]
    grad_sum = lax.optimization_barrier(jnp.sum(grad_std, axis=1))
    grad_proj = lax.optimization_barrier(jnp.sum(grad_std * centered, axis=1))
    coef_one = gain_row * factor
    coef_two = gain_row * factor ** 3 * grad_proj
    raw_grad = coef_one[:, None] * (grad_std - (grad_sum / fan_in)[:, None]) - coef_two[:, None] * centered
    weight_sq = lax.optimization_barrier(jnp.sum(weight * weight, axis=1))
    grad_sq = lax.optimization_barrier(jnp.sum(raw_grad * raw_grad, axis=1))
    return apply_update(weight, momentum, raw_grad, weight_sq, grad_sq)

def reference(block_input, output_grad, conv_weight, conv_gain, conv_momentum, proj_weight, proj_gain, proj_momentum):
    conv_std, conv_cent, conv_factor = standardize(conv_weight, conv_gain)
    proj_std, proj_cent, proj_factor = standardize(proj_weight, proj_gain)
    groups = CH // GW
    kernel = conv_std.reshape(groups, GW, 9, GW).astype(jnp.float32)
    image_count = block_input.shape[0]
    map_rows = block_input.shape[1]
    map_cols = block_input.shape[2]
    pixels = map_rows * map_cols

    def image_step(carry, inputs):
        conv_acc, proj_acc = carry
        image, cotangent = inputs
        activated = jax.nn.gelu(image.astype(jnp.float32)).astype(jnp.bfloat16)
        padded = jnp.pad(activated, ((1, 1), (1, 1), (0, 0)))
        patch_list = []
        pre_act = jnp.zeros((pixels, groups, GW), jnp.float32)
        for position in range(9):
            top = position // 3
            left = position % 3
            patch = padded[top:top + map_rows, left:left + map_cols].reshape(pixels, groups, GW).astype(jnp.float32)
            patch_list.append(patch)
            pre_act = pre_act + jnp.einsum('pgi,goi->pgo', patch, kernel[:, :, position, :])
        pre_flat = pre_act.reshape(pixels, CH)
        hidden = jax.nn.gelu(pre_flat).astype(jnp.bfloat16)
        upstream = cotangent.reshape(pixels, OUT)
        hidden_grad = jnp.dot(upstream, proj_std, preferred_element_type=jnp.float32)
        pre_grad = (hidden_grad * gelu_slope(pre_flat)).astype(jnp.bfloat16)
        proj_acc = proj_acc + jnp.einsum('po,pi->oi', upstream.astype(jnp.float32), hidden.astype(jnp.float32))
        grad_groups = pre_grad.reshape(pixels, groups, GW).astype(jnp.float32)
        conv_terms = jnp.stack([jnp.einsum('pgi,pgo->goi', patch, grad_groups) for patch in patch_list], axis=2)
        conv_acc = conv_acc + conv_terms.reshape(CH, 9 * GW)
        grad_pad = jnp.pad(pre_grad.reshape(map_rows, map_cols, CH), ((1, 1), (1, 1), (0, 0)))
        act_grad = jnp.zeros((pixels, groups, GW), jnp.float32)
        for position in range(9):
            top = 2 - position // 3
            left = 2 - position % 3
            piece = grad_pad[top:top + map_rows, left:left + map_cols].reshape(pixels, groups, GW).astype(jnp.float32)
            act_grad = act_grad + jnp.einsum('pgo,goi->pgi', piece, kernel[:, :, position, :])
        slope = gelu_slope(image.astype(jnp.float32))
        input_grad = (act_grad.reshape(map_rows, map_cols, CH) * slope).astype(jnp.bfloat16)
        return ((conv_acc, proj_acc), input_grad)
    start = (jnp.zeros((CH, 9 * GW), jnp.float32), jnp.zeros((OUT, CH), jnp.float32))
    (conv_acc, proj_acc), input_grad = lax.scan(image_step, start, (block_input, output_grad))
    conv_grad = conv_acc / image_count
    proj_grad = proj_acc / image_count
    new_conv_weight, new_conv_momentum = update(conv_weight, conv_gain, conv_momentum, conv_cent, conv_factor, conv_grad)
    new_proj_weight, new_proj_momentum = update(proj_weight, proj_gain, proj_momentum, proj_cent, proj_factor, proj_grad)
    return (input_grad, new_conv_weight, new_conv_momentum, new_proj_weight, new_proj_momentum)
```

```python
import functools
import math

import jax
import jax.numpy as jnp
from jax import lax
from jax.experimental import pallas as pl
from jax.experimental.pallas import tpu as pltpu
from jax.sharding import PartitionSpec as P

ws_eps = 0.0001
clip_ratio = 0.05
momentum_rate = 0.9
learn_rate = 1.6
norm_eps = 1e-06

F32 = jnp.float32
BF16 = jnp.bfloat16
MESH = pl.DeviceIdType.MESH
TAPS = 3
C0 = math.sqrt(2.0 / math.pi)
C1 = 0.044715


def gelu_parts(x):
    t = jnp.tanh(C0 * (x + C1 * (x * x * x)))
    half = 0.5 * (1.0 + t)
    slope = half + (0.5 * C0) * x * (1.0 - t * t) * (1.0 + (3.0 * C1) * (x * x))
    return x * half, slope


def dot_nn(a, b):
    return jnp.dot(a, b, preferred_element_type=F32)


def dot_nt(a, b):
    return lax.dot_general(a, b, (((1,), (1,)), ((), ())), preferred_element_type=F32)


def dot_tn(a, b):
    return lax.dot_general(a, b, (((0,), (0,)), ((), ())), preferred_element_type=F32)


def row_blocks(nc, np_, nblk):
    return [(0, nc)] + [(nc + b * np_, np_) for b in range(nblk)]


def bit_of(me, k):
    return (me // 2**k) % 2


def partner_of(me, k):
    return me + (1 - 2 * bit_of(me, k)) * 2**k


def greet(n):
    me = lax.axis_index("batch")
    r = lax.axis_index("rows")
    barrier = pltpu.get_barrier_semaphore()
    for d in range(1, n):
        pl.semaphore_signal(
            barrier, inc=1, device_id={"batch": (me + d) % n}, device_id_type=MESH
        )
    pl.semaphore_signal(barrier, inc=1, device_id={"rows": 1 - r}, device_id_type=MESH)
    pl.semaphore_wait(barrier, n)


def push_all(n, me, src, slots, send, recv):
    copies = []
    for d in range(1, n):
        copy = pltpu.make_async_remote_copy(
            src_ref=src,
            dst_ref=slots.at[me],
            send_sem=send.at[d - 1],
            recv_sem=recv.at[d - 1],
            device_id={"batch": (me + d) % n},
            device_id_type=MESH,
        )
        copy.start()
        copies.append(copy)
    slots[me] = src[...]
    for copy in copies:
        copy.wait()


def merged(n, slots, at, at_sq, counts, fan):
    total = slots[0, at : at + 1]
    for i in range(1, n):
        total = total + slots[i, at : at + 1]
    mean = total / fan
    spread = None
    for i in range(n):
        off = slots[i, at : at + 1] / counts - mean
        term = slots[i, at_sq : at_sq + 1] + counts * (off * off)
        spread = term if spread is None else spread + term
    return total, mean, spread


def gather_kernel(n, nb, blocks, edge_x, edge_u, w_ref, gain_ref, x_ref, u_ref,
                  full_ref, stat_ref, hx_ref, hu_ref,
                  src, slots, s_send, s_recv, g_send, g_recv, h_send, h_recv):
    me = lax.axis_index("batch")
    r = lax.axis_index("rows")
    greet(n)
    halos = []
    for at, (ref, out, width) in enumerate(((x_ref, hx_ref, edge_x), (u_ref, hu_ref, edge_u))):
        first = (1 - r) * (ref.shape[0] - width)
        copy = pltpu.make_async_remote_copy(
            src_ref=ref.at[pl.ds(first, width)],
            dst_ref=out,
            send_sem=h_send.at[at],
            recv_sem=h_recv.at[at],
            device_id={"rows": 1 - r},
            device_id_type=MESH,
        )
        copy.start()
        halos.append(copy)
    w = w_ref[...]
    src[...] = jnp.zeros_like(src)
    kinds = len(blocks)
    for b, (first, count) in enumerate(blocks):
        piece = w[first : first + count]
        s = jnp.sum(piece, axis=0, keepdims=True)
        cent = piece - s / count
        src[b : b + 1] = s
        src[kinds + b : kinds + b + 1] = jnp.sum(cent * cent, axis=0, keepdims=True)
    push_all(n, me, src, slots, s_send, s_recv)
    pos = 0
    for k in range(nb):
        pos = pos + bit_of(me, k) * 2 ** (nb - 1 - k)
    stat_ref[...] = jnp.zeros_like(stat_ref)
    for b, (first, count) in enumerate(blocks):
        _, mean, spread = merged(n, slots, b, kinds + b, count, n * count)
        stat_ref[b : b + 1] = mean
        stat_ref[kinds + b : kinds + b + 1] = spread
        scale = gain_ref[b : b + 1] * lax.rsqrt(spread + ws_eps)
        full_ref[pos, first : first + count] = (scale * (w[first : first + count] - mean)).astype(BF16)
    for step in range(nb):
        k = nb - 1 - step
        size = 2**step
        base = (pos // size) * size
        copy = pltpu.make_async_remote_copy(
            src_ref=full_ref.at[pl.ds(base, size)],
            dst_ref=full_ref.at[pl.ds(base, size)],
            send_sem=g_send.at[step],
            recv_sem=g_recv.at[step],
            device_id={"batch": partner_of(me, k)},
            device_id_type=MESH,
        )
        copy.start()
        copy.wait()
    for copy in halos:
        copy.wait()


def reduce_kernel(n, nb, images, blocks, part_ref, w_ref, m_ref, stat_ref, gain_ref,
                  new_w_ref, new_m_ref, *scratch):
    recvs = scratch[:nb]
    accs = scratch[nb : 2 * nb]
    recv_x, src, slots, r_send, r_recv, s_send, s_recv, x_send, x_recv = scratch[2 * nb :]
    me = lax.axis_index("batch")
    r = lax.axis_index("rows")
    greet(n)
    cur = part_ref
    for k in range(nb):
        h = n >> (k + 1)
        bit = bit_of(me, k)
        copy = pltpu.make_async_remote_copy(
            src_ref=cur.at[pl.ds((1 - bit) * h, h)],
            dst_ref=recvs[k],
            send_sem=r_send.at[k],
            recv_sem=r_recv.at[k],
            device_id={"batch": partner_of(me, k)},
            device_id_type=MESH,
        )
        copy.start()
        copy.wait()
        acc = accs[k]

        def add(i, carry, cur=cur, acc=acc, rec=recvs[k], first=bit * h):
            acc[i] = (cur[first + i].astype(F32) + rec[i].astype(F32)).astype(acc.dtype)
            return carry

        lax.fori_loop(0, h, add, 0)
        cur = acc
    copy = pltpu.make_async_remote_copy(
        src_ref=cur, dst_ref=recv_x, send_sem=x_send, recv_sem=x_recv,
        device_id={"rows": 1 - r}, device_id_type=MESH,
    )
    copy.start()
    copy.wait()
    grad = (cur[0] + recv_x[0]) / images
    w = w_ref[...]
    kinds = len(blocks)
    src[...] = jnp.zeros_like(src)
    for b, (first, count) in enumerate(blocks):
        piece = grad[first : first + count]
        cent = w[first : first + count] - stat_ref[b : b + 1]
        s = jnp.sum(piece, axis=0, keepdims=True)
        off = piece - s / count
        src[b : b + 1] = s
        src[kinds + b : kinds + b + 1] = jnp.sum(off * off, axis=0, keepdims=True)
        src[2 * kinds + b : 2 * kinds + b + 1] = jnp.sum(piece * cent, axis=0, keepdims=True)
    push_all(n, me, src, slots, s_send, s_recv)
    for b, (first, count) in enumerate(blocks):
        fan = n * count
        _, gmean, gspread = merged(n, slots, b, kinds + b, count, fan)
        at = 2 * kinds + b
        proj = slots[0, at : at + 1]
        for i in range(1, n):
            proj = proj + slots[i, at : at + 1]
        mean = stat_ref[b : b + 1]
        spread = stat_ref[kinds + b : kinds + b + 1]
        factor = lax.rsqrt(spread + ws_eps)
        f2 = factor * factor
        one = gain_ref[b : b + 1] * factor
        two = one * f2 * proj
        grad_sq = one * one * jnp.maximum(gspread - f2 * proj * proj * (2.0 - f2 * spread), 0.0)
        weight_sq = spread + fan * (mean * mean)
        clip = jnp.minimum(1.0, clip_ratio * jnp.sqrt(weight_sq) * lax.rsqrt(grad_sq + norm_eps))
        wp = w[first : first + count]
        raw = one * (grad[first : first + count] - gmean) - two * (wp - mean)
        clipped = clip * raw
        new_m = momentum_rate * m_ref[first : first + count] + clipped
        new_m_ref[first : first + count] = new_m
        new_w_ref[first : first + count] = wp - learn_rate * (clipped + momentum_rate * new_m)


def shifted(vals, step, mc):
    rows = vals.shape[0]
    col = lax.broadcasted_iota(jnp.int32, vals.shape, 0)
    if step > 0:
        return jnp.where(col == mc - 1, 0.0, pltpu.roll(vals, rows - 1, 0))
    return jnp.where(col == 0, 0.0, pltpu.roll(vals, 1, 0))


def compute_kernel(n, order, mr, mc, gw, nc, np_, nblk,
                   x_ref, u_ref, hx_ref, hu_ref, full_ref,
                   ig_ref, part_ref,
                   kt, pt, xs, ys, hid, cg, pg):
    ch = x_ref.shape[1]
    groups = ch // gw
    wide = TAPS * gw
    px = mr * mc
    r = lax.axis_index("rows")
    for d in range(n):
        kt[d * nc : (d + 1) * nc] = full_ref[order[d], :nc]
        for b in range(nblk):
            pt[d * np_ : (d + 1) * np_, b * ch : (b + 1) * ch] = full_ref[
                order[d], nc + b * np_ : nc + (b + 1) * np_
            ]

    def place(at, vals):
        act = gelu_parts(vals)[0].astype(BF16).astype(F32)
        for j in range(TAPS):
            moved = act if j == 1 else shifted(act, j - 1, mc)
            moved = moved.astype(BF16)
            for g in range(groups):
                xs[pl.ds(at, mc), g * wide + j * gw : g * wide + (j + 1) * gw] = moved[
                    :, g * gw : (g + 1) * gw
                ]

    for e in range(2):
        edge = hx_ref[e * mc : (e + 1) * mc].astype(F32)
        place(e * mc, jnp.where(r == 1, edge, 0.0))
        place((mr + 2 + e) * mc, jnp.where(r == 0, edge, 0.0))

    def body(row, carry):
        at = pl.multiple_of(row * mc, mc)
        place(pl.multiple_of(at + 2 * mc, mc), x_ref[pl.ds(at, mc)].astype(F32))
        return carry

    lax.fori_loop(0, mr, body, 0)

    def forward(e, up):
        hg = dot_nt(up, pt[...])
        for g in range(groups):
            acc = None
            for i in range(TAPS):
                term = dot_nn(
                    xs[pl.ds(pl.multiple_of((e + i) * mc, mc), up.shape[0]), g * wide : (g + 1) * wide],
                    kt[i * wide : (i + 1) * wide, g * gw : (g + 1) * gw],
                )
                acc = term if acc is None else acc + term
            h, slope = gelu_parts(acc)
            hid[pl.ds(pl.multiple_of(e * mc, mc), up.shape[0]), g * gw : (g + 1) * gw] = h.astype(BF16)
            grad = (hg[:, g * gw : (g + 1) * gw] * slope).astype(BF16).astype(F32)
            for q in range(up.shape[0] // mc):
                here = grad[q * mc : (q + 1) * mc]
                for j in range(TAPS):
                    moved = here if j == 1 else shifted(here, 1 - j, mc)
                    ys[pl.ds(pl.multiple_of((e + q) * mc, mc), mc), g * wide + j * gw : g * wide + (j + 1) * gw] = moved.astype(BF16)

    edge = hu_ref[...].astype(F32)
    forward(0, jnp.where(r == 1, edge, 0.0).astype(BF16))
    forward(mr + 1, jnp.where(r == 0, edge, 0.0).astype(BF16))
    many = 2 if mr % 2 == 0 else 1

    def fwd(t, carry):
        up = u_ref[pl.ds(pl.multiple_of(t * many * mc, mc), many * mc)]
        forward(1 + t * many, up)
        return carry

    lax.fori_loop(0, mr // many, fwd, 0)

    pg[...] = dot_tn(hid[mc : mc + px], u_ref[...])
    for g in range(groups):
        own = ys[mc : mc + px, g * wide + gw : g * wide + 2 * gw]
        for i in range(TAPS):
            cg[i * wide : (i + 1) * wide, g * gw : (g + 1) * gw] = dot_tn(
                xs[(1 + i) * mc : (1 + i) * mc + px, g * wide : (g + 1) * wide], own
            )
    for d in range(n):
        part_ref[order[d], :nc] = cg[d * nc : (d + 1) * nc].astype(BF16)
        for b in range(nblk):
            part_ref[order[d], nc + b * np_ : nc + (b + 1) * np_] = pg[
                d * np_ : (d + 1) * np_, b * ch : (b + 1) * ch
            ].astype(BF16)

    def back(t, carry):
        at = pl.multiple_of(t * many * mc, mc)
        for g in range(groups):
            acc = None
            for i in range(TAPS):
                for j in range(TAPS):
                    term = dot_nt(
                        ys[pl.ds(pl.multiple_of(at + (2 - i) * mc, mc), many * mc), g * wide + j * gw : g * wide + (j + 1) * gw],
                        kt[i * wide + j * gw : i * wide + (j + 1) * gw, g * gw : (g + 1) * gw],
                    )
                    acc = term if acc is None else acc + term
            slope = gelu_parts(x_ref[pl.ds(at, many * mc), g * gw : (g + 1) * gw].astype(F32))[1]
            ig_ref[pl.ds(at, many * mc), g * gw : (g + 1) * gw] = (acc * slope).astype(BF16)
        return carry

    lax.fori_loop(0, mr // many, back, 0)


def local(n, nrows, block_input, output_grad, conv_weight, conv_gain, conv_momentum,
          proj_weight, proj_gain, proj_momentum):
    assert nrows == 2
    nb = n.bit_length() - 1
    assert 2**nb == n
    _, mr, mc, ch = block_input.shape
    out = output_grad.shape[3]
    nc = conv_weight.shape[1]
    np_ = proj_weight.shape[1]
    nblk = out // ch
    gw = nc * n // (TAPS * TAPS)
    rows = nc + nblk * np_
    blocks = row_blocks(nc, np_, nblk)
    kinds = len(blocks)
    order = [int(format(d, "0%db" % nb)[::-1], 2) for d in range(n)]
    px = mr * mc

    def packed(conv, proj):
        return jnp.concatenate(
            [conv.T] + [proj[b * ch : (b + 1) * ch].T for b in range(nblk)], axis=0
        )

    def unpacked(both):
        conv = both[:nc].T
        proj = jnp.concatenate(
            [both[nc + b * np_ : nc + (b + 1) * np_].T for b in range(nblk)], axis=0
        )
        return conv, proj

    w = packed(conv_weight, proj_weight)
    m = packed(conv_momentum, proj_momentum)
    gain = jnp.concatenate([conv_gain[None], proj_gain.reshape(nblk, ch)], axis=0)
    x = block_input.reshape(px, ch)
    u = output_grad.reshape(px, out)
    vmem = pl.BlockSpec(memory_space=pltpu.VMEM)
    sdt = jax.ShapeDtypeStruct
    stat_rows = -(-2 * kinds // 8) * 8
    grad_rows = -(-3 * kinds // 8) * 8
    dma = pltpu.SemaphoreType.DMA
    full, stat, hx, hu = pl.pallas_call(
        functools.partial(gather_kernel, n, nb, blocks, 2 * mc, mc),
        out_shape=(
            sdt((n, rows, ch), BF16),
            sdt((stat_rows, ch), F32),
            sdt((2 * mc, ch), BF16),
            sdt((mc, out), BF16),
        ),
        in_specs=[vmem] * 4,
        out_specs=(vmem,) * 4,
        scratch_shapes=[
            pltpu.VMEM((stat_rows, ch), F32),
            pltpu.VMEM((n, stat_rows, ch), F32),
            dma((n - 1,)), dma((n - 1,)),
            dma((nb,)), dma((nb,)),
            dma((2,)), dma((2,)),
        ],
        compiler_params=pltpu.CompilerParams(collective_id=0, has_side_effects=True),
        name="gather",
    )(w, gain, x, u)
    ig, part = pl.pallas_call(
        functools.partial(compute_kernel, n, order, mr, mc, gw, nc, np_, nblk),
        out_shape=(sdt((px, ch), BF16), sdt((n, rows, ch), BF16)),
        in_specs=[vmem] * 5,
        out_specs=(vmem,) * 2,
        scratch_shapes=[
            pltpu.VMEM((n * nc, ch), BF16),
            pltpu.VMEM((n * np_, out), BF16),
            pltpu.VMEM(((mr + 4) * mc, TAPS * ch), BF16),
            pltpu.VMEM(((mr + 2) * mc, TAPS * ch), BF16),
            pltpu.VMEM(((mr + 2) * mc, ch), BF16),
            pltpu.VMEM((n * nc, ch), F32),
            pltpu.VMEM((n * np_, out), F32),
        ],
        name="compute",
    )(x, u, hx, hu, full)
    halves = [n >> (k + 1) for k in range(nb)]
    new_w, new_m = pl.pallas_call(
        functools.partial(reduce_kernel, n, nb, n, blocks),
        out_shape=(sdt((rows, ch), F32), sdt((rows, ch), F32)),
        in_specs=[vmem] * 5,
        out_specs=(vmem,) * 2,
        scratch_shapes=[pltpu.VMEM((h, rows, ch), BF16) for h in halves]
        + [pltpu.VMEM((h, rows, ch), BF16 if h > 1 else F32) for h in halves]
        + [
            pltpu.VMEM((1, rows, ch), F32),
            pltpu.VMEM((grad_rows, ch), F32),
            pltpu.VMEM((n, grad_rows, ch), F32),
            dma((nb,)), dma((nb,)),
            dma((n - 1,)), dma((n - 1,)),
            dma, dma,
        ],
        compiler_params=pltpu.CompilerParams(collective_id=1, has_side_effects=True),
        name="reduce",
    )(part, w, m, stat, gain)
    new_conv_w, new_proj_w = unpacked(new_w)
    new_conv_m, new_proj_m = unpacked(new_m)
    return (ig.reshape(block_input.shape), new_conv_w, new_conv_m, new_proj_w, new_proj_m)


def solution(mesh):
    in_specs = (
        P("batch", "rows", None, None),
        P("batch", "rows", None, None),
        P(None, "batch"),
        P(),
        P(None, "batch"),
        P(None, "batch"),
        P(),
        P(None, "batch"),
    )
    out_specs = (
        P("batch", "rows", None, None),
        P(None, "batch"),
        P(None, "batch"),
        P(None, "batch"),
        P(None, "batch"),
    )
    body = functools.partial(local, mesh.shape["batch"], mesh.shape["rows"])
    return jax.shard_map(body, mesh=mesh, in_specs=in_specs, out_specs=out_specs, check_vma=False)
```

```python
import functools
import math

import jax
import jax.numpy as jnp
from jax import lax
from jax.experimental import pallas as pl
from jax.experimental.pallas import tpu as pltpu
from jax.sharding import PartitionSpec as P

ws_eps = 0.0001
clip_ratio = 0.05
momentum_rate = 0.9
learn_rate = 1.6
norm_eps = 1e-06

F32 = jnp.float32
BF16 = jnp.bfloat16
MESH = pl.DeviceIdType.MESH
TAPS = 3
C0 = math.sqrt(2.0 / math.pi)
C1 = 0.044715


def gelu_parts(x):
    t = jnp.tanh(C0 * (x + C1 * (x * x * x)))
    half = 0.5 * (1.0 + t)
    slope = half + (0.5 * C0) * x * (1.0 - t * t) * (1.0 + (3.0 * C1) * (x * x))
    return x * half, slope


def dot_nn(a, b):
    return jnp.dot(a, b, preferred_element_type=F32)


def dot_nt(a, b):
    return lax.dot_general(a, b, (((1,), (1,)), ((), ())), preferred_element_type=F32)


def dot_tn(a, b):
    return lax.dot_general(a, b, (((0,), (0,)), ((), ())), preferred_element_type=F32)


def bit_of(me, k):
    return (me // 2**k) % 2


def partner_of(me, k):
    return me + (1 - 2 * bit_of(me, k)) * 2**k


def greet_signal(n):
    me = lax.axis_index("batch")
    r = lax.axis_index("rows")
    barrier = pltpu.get_barrier_semaphore()
    for d in range(1, n):
        pl.semaphore_signal(
            barrier, inc=1, device_id={"batch": (me + d) % n}, device_id_type=MESH
        )
    pl.semaphore_signal(barrier, inc=1, device_id={"rows": 1 - r}, device_id_type=MESH)


def greet_wait(n):
    pl.semaphore_wait(pltpu.get_barrier_semaphore(), n)


def push_start(n, me, src, slots, send, recv):
    copies = []
    for d in range(1, n):
        copy = pltpu.make_async_remote_copy(
            src_ref=src,
            dst_ref=slots.at[me],
            send_sem=send.at[d - 1],
            recv_sem=recv.at[d - 1],
            device_id={"batch": (me + d) % n},
            device_id_type=MESH,
        )
        copy.start()
        copies.append(copy)
    slots[me] = src[...]
    return copies


def merged(n, slots, at, at_sq, counts, fan):
    total = slots[0, at : at + 1]
    for i in range(1, n):
        total = total + slots[i, at : at + 1]
    mean = total / fan
    spread = None
    for i in range(n):
        off = slots[i, at : at + 1] / counts - mean
        term = slots[i, at_sq : at_sq + 1] + counts * (off * off)
        spread = term if spread is None else spread + term
    return total, mean, spread


LANE = 128


def kind_slices(ch, out):
    return [(0, 0)] + [(1, b * ch) for b in range(out // ch)]


def gather_kernel(n, nb, pieces, edge_x, edge_u, wc_ref, wp_ref, gc_ref, gp_ref, x_ref, u_ref,
                  full_ref, stat_ref, hx_ref, hu_ref,
                  src, slots, s_send, s_recv, g_send, g_recv, h_send, h_recv):
    me = lax.axis_index("batch")
    r = lax.axis_index("rows")
    greet_signal(n)
    ch = wc_ref.shape[1]
    kinds = kind_slices(ch, wp_ref.shape[1])
    nk = len(kinds)
    w_refs = (wc_ref, wp_ref)
    gain_refs = (gc_ref, gp_ref)
    src[...] = jnp.zeros_like(src)
    for b, (which, col) in enumerate(kinds):
        piece = w_refs[which][:, col : col + ch]
        s = jnp.sum(piece, axis=0, keepdims=True)
        cent = piece - s / piece.shape[0]
        src[b : b + 1] = s
        src[nk + b : nk + b + 1] = jnp.sum(cent * cent, axis=0, keepdims=True)
    greet_wait(n)
    push = push_start(n, me, src, slots, s_send, s_recv)
    halos = []
    for at, (ref, out, width) in enumerate(((x_ref, hx_ref, edge_x), (u_ref, hu_ref, edge_u))):
        first = (1 - r) * (ref.shape[0] - width)
        copy = pltpu.make_async_remote_copy(
            src_ref=ref.at[pl.ds(first, width)],
            dst_ref=out,
            send_sem=h_send.at[at],
            recv_sem=h_recv.at[at],
            device_id={"rows": 1 - r},
            device_id_type=MESH,
        )
        copy.start()
        halos.append(copy)
    for copy in push:
        copy.wait()
    pos = 0
    for k in range(nb):
        pos = pos + bit_of(me, k) * 2 ** (nb - 1 - k)
    stat_ref[...] = jnp.zeros_like(stat_ref)
    first = 0
    for b, (which, col) in enumerate(kinds):
        count = w_refs[which].shape[0]
        _, mean, spread = merged(n, slots, b, nk + b, count, n * count)
        stat_ref[b : b + 1] = mean
        stat_ref[nk + b : nk + b + 1] = spread
        scale = gain_refs[which][:, col : col + ch] * lax.rsqrt(spread + ws_eps)
        std = (scale * (w_refs[which][:, col : col + ch] - mean)).astype(BF16)
        for p in range(pieces):
            full_ref[p, pos, first : first + count] = std[:, p * LANE : (p + 1) * LANE]
        first += count
    flight = [None] * pieces
    for t in range(nb + pieces):
        for p in range(pieces):
            step = t - p
            if step < 0 or step > nb:
                continue
            if flight[p] is not None:
                flight[p].wait()
            if step == nb:
                continue
            size = 2**step
            base = (pos // size) * size
            flight[p] = pltpu.make_async_remote_copy(
                src_ref=full_ref.at[p, pl.ds(base, size)],
                dst_ref=full_ref.at[p, pl.ds(base, size)],
                send_sem=g_send.at[p, step],
                recv_sem=g_recv.at[p, step],
                device_id={"batch": partner_of(me, nb - 1 - step)},
                device_id_type=MESH,
            )
            flight[p].start()
    for copy in halos:
        copy.wait()


def reduce_kernel(n, nb, pieces, images, part_ref, wc_ref, wp_ref, mc_ref, mp_ref, stat_ref,
                  gc_ref, gp_ref, nwc_ref, nwp_ref, nmc_ref, nmp_ref, *scratch):
    recvs = scratch[:nb]
    accs = scratch[nb : 2 * nb]
    recv_x, src, slots, r_send, r_recv, s_send, s_recv, x_send, x_recv = scratch[2 * nb :]
    me = lax.axis_index("batch")
    r = lax.axis_index("rows")
    greet_signal(n)
    greet_wait(n)
    flight = [None] * pieces
    for t in range(nb + 1 + pieces):
        for p in range(pieces):
            k = t - p
            if k < 0 or k > nb + 1:
                continue
            if flight[p] is not None:
                flight[p].wait()
            if 1 <= k <= nb:
                h = n >> k
                cur = part_ref if k == 1 else accs[k - 2]
                acc = accs[k - 1]
                rec = recvs[k - 1]
                lo = bit_of(me, k - 1) * h

                def add(i, carry, cur=cur, acc=acc, rec=rec, lo=lo, p=p):
                    acc[p, i] = (cur[p, lo + i].astype(F32) + rec[p, i].astype(F32)).astype(acc.dtype)
                    return carry

                lax.fori_loop(0, h, add, 0)
            if k < nb:
                h = n >> (k + 1)
                cur = part_ref if k == 0 else accs[k - 1]
                flight[p] = pltpu.make_async_remote_copy(
                    src_ref=cur.at[p, pl.ds((1 - bit_of(me, k)) * h, h)],
                    dst_ref=recvs[k].at[p],
                    send_sem=r_send.at[p, k],
                    recv_sem=r_recv.at[p, k],
                    device_id={"batch": partner_of(me, k)},
                    device_id_type=MESH,
                )
                flight[p].start()
            elif k == nb:
                flight[p] = pltpu.make_async_remote_copy(
                    src_ref=accs[nb - 1].at[p],
                    dst_ref=recv_x.at[p],
                    send_sem=x_send.at[p],
                    recv_sem=x_recv.at[p],
                    device_id={"rows": 1 - r},
                    device_id_type=MESH,
                )
                flight[p].start()
    last = accs[nb - 1]
    grad = jnp.concatenate([last[p, 0] + recv_x[p, 0] for p in range(pieces)], axis=1) / images
    ch = wc_ref.shape[1]
    kinds = kind_slices(ch, wp_ref.shape[1])
    nk = len(kinds)
    w_refs = (wc_ref, wp_ref)
    gain_refs = (gc_ref, gp_ref)
    src[...] = jnp.zeros_like(src)
    parts = []
    first = 0
    for b, (which, col) in enumerate(kinds):
        count = w_refs[which].shape[0]
        piece = grad[first : first + count]
        parts.append(piece)
        first += count
        cent = w_refs[which][:, col : col + ch] - stat_ref[b : b + 1]
        s = jnp.sum(piece, axis=0, keepdims=True)
        off = piece - s / count
        src[b : b + 1] = s
        src[nk + b : nk + b + 1] = jnp.sum(off * off, axis=0, keepdims=True)
        src[2 * nk + b : 2 * nk + b + 1] = jnp.sum(piece * cent, axis=0, keepdims=True)
    for copy in push_start(n, me, src, slots, s_send, s_recv):
        copy.wait()
    for b, (which, col) in enumerate(kinds):
        count = w_refs[which].shape[0]
        cols = slice(col, col + ch)
        fan = n * count
        _, gmean, gspread = merged(n, slots, b, nk + b, count, fan)
        at = 2 * nk + b
        proj = slots[0, at : at + 1]
        for i in range(1, n):
            proj = proj + slots[i, at : at + 1]
        mean = stat_ref[b : b + 1]
        spread = stat_ref[nk + b : nk + b + 1]
        factor = lax.rsqrt(spread + ws_eps)
        f2 = factor * factor
        one = gain_refs[which][:, cols] * factor
        two = one * f2 * proj
        grad_sq = one * one * jnp.maximum(gspread - f2 * proj * proj * (2.0 - f2 * spread), 0.0)
        weight_sq = spread + fan * (mean * mean)
        clip = jnp.minimum(1.0, clip_ratio * jnp.sqrt(weight_sq) * lax.rsqrt(grad_sq + norm_eps))
        wp = w_refs[which][:, cols]
        clipped = clip * (one * (parts[b] - gmean) - two * (wp - mean))
        new_m = momentum_rate * (mc_ref, mp_ref)[which][:, cols] + clipped
        (nmc_ref, nmp_ref)[which][:, cols] = new_m
        (nwc_ref, nwp_ref)[which][:, cols] = wp - learn_rate * (clipped + momentum_rate * new_m)


def shifted(vals, step, mc):
    rows = vals.shape[0]
    col = lax.broadcasted_iota(jnp.int32, vals.shape, 0)
    if step > 0:
        return jnp.where(col == mc - 1, 0.0, pltpu.roll(vals, rows - 1, 0))
    return jnp.where(col == 0, 0.0, pltpu.roll(vals, 1, 0))


def compute_kernel(n, order, mr, mc, gw, nc, np_, nblk,
                   x_ref, u_ref, hx_ref, hu_ref, full_ref,
                   ig_ref, part_ref,
                   kt, pt, xs, ys, hid, cg, pg):
    ch = x_ref.shape[1]
    groups = ch // gw
    wide = TAPS * gw
    px = mr * mc
    r = lax.axis_index("rows")
    for d in range(n):
        for p in range(ch // LANE):
            kt[d * nc : (d + 1) * nc, p * LANE : (p + 1) * LANE] = full_ref[p, order[d], :nc]
            for b in range(nblk):
                at = b * ch + p * LANE
                pt[d * np_ : (d + 1) * np_, at : at + LANE] = full_ref[
                    p, order[d], nc + b * np_ : nc + (b + 1) * np_
                ]

    def place(at, vals):
        act = gelu_parts(vals)[0].astype(BF16).astype(F32)
        for j in range(TAPS):
            moved = act if j == 1 else shifted(act, j - 1, mc)
            moved = moved.astype(BF16)
            for g in range(groups):
                xs[pl.ds(at, mc), g * wide + j * gw : g * wide + (j + 1) * gw] = moved[
                    :, g * gw : (g + 1) * gw
                ]

    for e in range(2):
        edge = hx_ref[e * mc : (e + 1) * mc].astype(F32)
        place(e * mc, jnp.where(r == 1, edge, 0.0))
        place((mr + 2 + e) * mc, jnp.where(r == 0, edge, 0.0))

    def body(row, carry):
        at = pl.multiple_of(row * mc, mc)
        place(pl.multiple_of(at + 2 * mc, mc), x_ref[pl.ds(at, mc)].astype(F32))
        return carry

    lax.fori_loop(0, mr, body, 0)

    def forward(e, up):
        hg = dot_nt(up, pt[...])
        for g in range(groups):
            acc = None
            for i in range(TAPS):
                term = dot_nn(
                    xs[pl.ds(pl.multiple_of((e + i) * mc, mc), up.shape[0]), g * wide : (g + 1) * wide],
                    kt[i * wide : (i + 1) * wide, g * gw : (g + 1) * gw],
                )
                acc = term if acc is None else acc + term
            h, slope = gelu_parts(acc)
            hid[pl.ds(pl.multiple_of(e * mc, mc), up.shape[0]), g * gw : (g + 1) * gw] = h.astype(BF16)
            grad = (hg[:, g * gw : (g + 1) * gw] * slope).astype(BF16).astype(F32)
            for q in range(up.shape[0] // mc):
                here = grad[q * mc : (q + 1) * mc]
                for j in range(TAPS):
                    moved = here if j == 1 else shifted(here, 1 - j, mc)
                    ys[pl.ds(pl.multiple_of((e + q) * mc, mc), mc), g * wide + j * gw : g * wide + (j + 1) * gw] = moved.astype(BF16)

    edge = hu_ref[...].astype(F32)
    forward(0, jnp.where(r == 1, edge, 0.0).astype(BF16))
    forward(mr + 1, jnp.where(r == 0, edge, 0.0).astype(BF16))
    many = 2 if mr % 2 == 0 else 1

    def fwd(t, carry):
        up = u_ref[pl.ds(pl.multiple_of(t * many * mc, mc), many * mc)]
        forward(1 + t * many, up)
        return carry

    lax.fori_loop(0, mr // many, fwd, 0)

    pg[...] = dot_tn(hid[mc : mc + px], u_ref[...])
    for g in range(groups):
        own = ys[mc : mc + px, g * wide + gw : g * wide + 2 * gw]
        for i in range(TAPS):
            cg[i * wide : (i + 1) * wide, g * gw : (g + 1) * gw] = dot_tn(
                xs[(1 + i) * mc : (1 + i) * mc + px, g * wide : (g + 1) * wide], own
            )
    for d in range(n):
        for p in range(ch // LANE):
            part_ref[p, order[d], :nc] = cg[
                d * nc : (d + 1) * nc, p * LANE : (p + 1) * LANE
            ].astype(BF16)
            for b in range(nblk):
                at = b * ch + p * LANE
                part_ref[p, order[d], nc + b * np_ : nc + (b + 1) * np_] = pg[
                    d * np_ : (d + 1) * np_, at : at + LANE
                ].astype(BF16)

    def back(t, carry):
        at = pl.multiple_of(t * many * mc, mc)
        for g in range(groups):
            acc = None
            for i in range(TAPS):
                for j in range(TAPS):
                    term = dot_nt(
                        ys[pl.ds(pl.multiple_of(at + (2 - i) * mc, mc), many * mc), g * wide + j * gw : g * wide + (j + 1) * gw],
                        kt[i * wide + j * gw : i * wide + (j + 1) * gw, g * gw : (g + 1) * gw],
                    )
                    acc = term if acc is None else acc + term
            slope = gelu_parts(x_ref[pl.ds(at, many * mc), g * gw : (g + 1) * gw].astype(F32))[1]
            ig_ref[pl.ds(at, many * mc), g * gw : (g + 1) * gw] = (acc * slope).astype(BF16)
        return carry

    lax.fori_loop(0, mr // many, back, 0)


def local(n, nrows, block_input, output_grad, conv_weight, conv_gain, conv_momentum,
          proj_weight, proj_gain, proj_momentum):
    assert nrows == 2
    nb = n.bit_length() - 1
    assert 2**nb == n
    _, mr, mc, ch = block_input.shape
    out = output_grad.shape[3]
    nc = conv_weight.shape[1]
    np_ = proj_weight.shape[1]
    nblk = out // ch
    gw = nc * n // (TAPS * TAPS)
    rows = nc + nblk * np_
    kinds = 1 + nblk
    pieces = ch // LANE
    order = [int(format(d, "0%db" % nb)[::-1], 2) for d in range(n)]
    px = mr * mc

    wc, wp, mc_, mp = conv_weight.T, proj_weight.T, conv_momentum.T, proj_momentum.T
    gc, gp = conv_gain[None], proj_gain[None]
    x = block_input.reshape(px, ch)
    u = output_grad.reshape(px, out)
    vmem = pl.BlockSpec(memory_space=pltpu.VMEM)
    sdt = jax.ShapeDtypeStruct
    stat_rows = -(-2 * kinds // 8) * 8
    grad_rows = -(-3 * kinds // 8) * 8
    dma = pltpu.SemaphoreType.DMA
    full, stat, hx, hu = pl.pallas_call(
        functools.partial(gather_kernel, n, nb, pieces, 2 * mc, mc),
        out_shape=(
            sdt((pieces, n, rows, LANE), BF16),
            sdt((stat_rows, ch), F32),
            sdt((2 * mc, ch), BF16),
            sdt((mc, out), BF16),
        ),
        in_specs=[vmem] * 6,
        out_specs=(vmem,) * 4,
        scratch_shapes=[
            pltpu.VMEM((stat_rows, ch), F32),
            pltpu.VMEM((n, stat_rows, ch), F32),
            dma((n - 1,)), dma((n - 1,)),
            dma((pieces, nb)), dma((pieces, nb)),
            dma((2,)), dma((2,)),
        ],
        compiler_params=pltpu.CompilerParams(collective_id=0, has_side_effects=True),
        name="gather",
    )(wc, wp, gc, gp, x, u)
    ig, part = pl.pallas_call(
        functools.partial(compute_kernel, n, order, mr, mc, gw, nc, np_, nblk),
        out_shape=(sdt((px, ch), BF16), sdt((pieces, n, rows, LANE), BF16)),
        in_specs=[vmem] * 5,
        out_specs=(vmem,) * 2,
        scratch_shapes=[
            pltpu.VMEM((n * nc, ch), BF16),
            pltpu.VMEM((n * np_, out), BF16),
            pltpu.VMEM(((mr + 4) * mc, TAPS * ch), BF16),
            pltpu.VMEM(((mr + 2) * mc, TAPS * ch), BF16),
            pltpu.VMEM(((mr + 2) * mc, ch), BF16),
            pltpu.VMEM((n * nc, ch), F32),
            pltpu.VMEM((n * np_, out), F32),
        ],
        name="compute",
    )(x, u, hx, hu, full)
    halves = [n >> (k + 1) for k in range(nb)]
    nwc, nwp, nmc, nmp = pl.pallas_call(
        functools.partial(reduce_kernel, n, nb, pieces, n),
        out_shape=(sdt((nc, ch), F32), sdt((np_, out), F32)) * 2,
        in_specs=[vmem] * 8,
        out_specs=(vmem,) * 4,
        scratch_shapes=[pltpu.VMEM((pieces, h, rows, LANE), BF16) for h in halves]
        + [pltpu.VMEM((pieces, h, rows, LANE), BF16 if h > 1 else F32) for h in halves]
        + [
            pltpu.VMEM((pieces, 1, rows, LANE), F32),
            pltpu.VMEM((grad_rows, ch), F32),
            pltpu.VMEM((n, grad_rows, ch), F32),
            dma((pieces, nb)), dma((pieces, nb)),
            dma((n - 1,)), dma((n - 1,)),
            dma((pieces,)), dma((pieces,)),
        ],
        compiler_params=pltpu.CompilerParams(collective_id=1, has_side_effects=True),
        name="reduce",
    )(part, wc, wp, mc_, mp, stat, gc, gp)
    return (ig.reshape(block_input.shape), nwc.T, nmc.T, nwp.T, nmp.T)


def solution(mesh):
    in_specs = (
        P("batch", "rows", None, None),
        P("batch", "rows", None, None),
        P(None, "batch"),
        P(),
        P(None, "batch"),
        P(None, "batch"),
        P(),
        P(None, "batch"),
    )
    out_specs = (
        P("batch", "rows", None, None),
        P(None, "batch"),
        P(None, "batch"),
        P(None, "batch"),
        P(None, "batch"),
    )
    body = functools.partial(local, mesh.shape["batch"], mesh.shape["rows"])
    return jax.shard_map(body, mesh=mesh, in_specs=in_specs, out_specs=out_specs, check_vma=False)
```

```python
import functools
import math

import jax
import jax.numpy as jnp
from jax import lax
from jax.experimental import pallas as pl
from jax.experimental.pallas import tpu as pltpu
from jax.sharding import PartitionSpec as P

ws_eps = 0.0001
clip_ratio = 0.05
momentum_rate = 0.9
learn_rate = 1.6
norm_eps = 1e-06

F32 = jnp.float32
BF16 = jnp.bfloat16
MESH = pl.DeviceIdType.MESH
TAPS = 3
C0 = math.sqrt(2.0 / math.pi)
C1 = 0.044715


def gelu_parts(x):
    t = jnp.tanh(C0 * (x + C1 * (x * x * x)))
    half = 0.5 * (1.0 + t)
    slope = half + (0.5 * C0) * x * (1.0 - t * t) * (1.0 + (3.0 * C1) * (x * x))
    return x * half, slope


def dot_nn(a, b):
    return jnp.dot(a, b, preferred_element_type=F32)


def dot_nt(a, b):
    return lax.dot_general(a, b, (((1,), (1,)), ((), ())), preferred_element_type=F32)


def dot_tn(a, b):
    return lax.dot_general(a, b, (((0,), (0,)), ((), ())), preferred_element_type=F32)


def bit_of(me, k):
    return (me // 2**k) % 2


def partner_of(me, k):
    return me + (1 - 2 * bit_of(me, k)) * 2**k


def greet_signal(n):
    me = lax.axis_index("batch")
    r = lax.axis_index("rows")
    barrier = pltpu.get_barrier_semaphore()
    for d in range(1, n):
        pl.semaphore_signal(
            barrier, inc=1, device_id={"batch": (me + d) % n}, device_id_type=MESH
        )
    pl.semaphore_signal(barrier, inc=1, device_id={"rows": 1 - r}, device_id_type=MESH)


def greet_wait(n):
    pl.semaphore_wait(pltpu.get_barrier_semaphore(), n)


def push_start(n, me, src, slots, send, recv):
    copies = []
    for d in range(1, n):
        copy = pltpu.make_async_remote_copy(
            src_ref=src,
            dst_ref=slots.at[me],
            send_sem=send.at[d - 1],
            recv_sem=recv.at[d - 1],
            device_id={"batch": (me + d) % n},
            device_id_type=MESH,
        )
        copy.start()
        copies.append(copy)
    for row in range(src.shape[0]):
        slots[me, row] = src[row]
    return copies


def merged(n, slots, at, at_sq, counts, fan):
    total = slots[0, at]
    for i in range(1, n):
        total = total + slots[i, at]
    mean = total / fan
    spread = None
    for i in range(n):
        off = slots[i, at] / counts - mean
        term = slots[i, at_sq] + counts * (off * off)
        spread = term if spread is None else spread + term
    return total, mean, spread


LANE = 128


def kind_slices(ch, out):
    return [(0, 0)] + [(1, b * ch) for b in range(out // ch)]


def gather_kernel(n, nb, pieces, edge_x, edge_u, wc_ref, wp_ref, gc_ref, gp_ref, x_ref, u_ref,
                  full_ref, stat_ref, hx_ref, hu_ref,
                  src, slots, s_send, s_recv, g_send, g_recv, h_send, h_recv):
    me = lax.axis_index("batch")
    r = lax.axis_index("rows")
    greet_signal(n)
    ch = wc_ref.shape[1]
    kinds = kind_slices(ch, wp_ref.shape[1])
    nk = len(kinds)
    w_refs = (wc_ref, wp_ref)
    gain_refs = (gc_ref, gp_ref)
    for b, (which, col) in enumerate(kinds):
        piece = w_refs[which][:, col : col + ch]
        s = jnp.sum(piece, axis=0, keepdims=True)
        cent = piece - s / piece.shape[0]
        src[b] = s
        src[nk + b] = jnp.sum(cent * cent, axis=0, keepdims=True)
    greet_wait(n)
    push = push_start(n, me, src, slots, s_send, s_recv)
    halos = []
    for at, (ref, out, width) in enumerate(((x_ref, hx_ref, edge_x), (u_ref, hu_ref, edge_u))):
        first = (1 - r) * (ref.shape[0] - width)
        copy = pltpu.make_async_remote_copy(
            src_ref=ref.at[pl.ds(first, width)],
            dst_ref=out,
            send_sem=h_send.at[at],
            recv_sem=h_recv.at[at],
            device_id={"rows": 1 - r},
            device_id_type=MESH,
        )
        copy.start()
        halos.append(copy)
    for copy in push:
        copy.wait()
    pos = 0
    for k in range(nb):
        pos = pos + bit_of(me, k) * 2 ** (nb - 1 - k)
    stat_ref[...] = jnp.zeros_like(stat_ref)
    first = 0
    for b, (which, col) in enumerate(kinds):
        count = w_refs[which].shape[0]
        _, mean, spread = merged(n, slots, b, nk + b, count, n * count)
        stat_ref[b : b + 1] = mean
        stat_ref[nk + b : nk + b + 1] = spread
        scale = gain_refs[which][col : col + ch][None] * lax.rsqrt(spread + ws_eps)
        std = (scale * (w_refs[which][:, col : col + ch] - mean)).astype(BF16)
        for p in range(pieces):
            full_ref[p, pos, first : first + count] = std[:, p * LANE : (p + 1) * LANE]
        first += count
    flight = [None] * pieces
    for t in range(nb + pieces):
        for p in range(pieces):
            step = t - p
            if step < 0 or step > nb:
                continue
            if flight[p] is not None:
                flight[p].wait()
            if step == nb:
                continue
            size = 2**step
            base = (pos // size) * size
            flight[p] = pltpu.make_async_remote_copy(
                src_ref=full_ref.at[p, pl.ds(base, size)],
                dst_ref=full_ref.at[p, pl.ds(base, size)],
                send_sem=g_send.at[p, step],
                recv_sem=g_recv.at[p, step],
                device_id={"batch": partner_of(me, nb - 1 - step)},
                device_id_type=MESH,
            )
            flight[p].start()
    for copy in halos:
        copy.wait()


def reduce_kernel(n, nb, pieces, images, part_ref, wc_ref, wp_ref, stat_ref,
                  gc_ref, gp_ref, grad_ref, coef_ref, *scratch):
    recvs = scratch[:nb]
    accs = scratch[nb : 2 * nb]
    recv_x, src, slots, r_send, r_recv, s_send, s_recv, x_send, x_recv = scratch[2 * nb :]
    me = lax.axis_index("batch")
    r = lax.axis_index("rows")
    greet_signal(n)
    greet_wait(n)
    flight = [None] * pieces
    for t in range(nb + 1 + pieces):
        for p in range(pieces):
            k = t - p
            if k < 0 or k > nb + 1:
                continue
            if flight[p] is not None:
                flight[p].wait()
            if 1 <= k <= nb:
                h = n >> k
                cur = part_ref if k == 1 else accs[k - 2]
                acc = accs[k - 1]
                rec = recvs[k - 1]
                lo = bit_of(me, k - 1) * h

                def add(i, carry, cur=cur, acc=acc, rec=rec, lo=lo, p=p):
                    acc[p, i] = (cur[p, lo + i].astype(F32) + rec[p, i].astype(F32)).astype(acc.dtype)
                    return carry

                lax.fori_loop(0, h, add, 0)
            if k < nb:
                h = n >> (k + 1)
                cur = part_ref if k == 0 else accs[k - 1]
                flight[p] = pltpu.make_async_remote_copy(
                    src_ref=cur.at[p, pl.ds((1 - bit_of(me, k)) * h, h)],
                    dst_ref=recvs[k].at[p],
                    send_sem=r_send.at[p, k],
                    recv_sem=r_recv.at[p, k],
                    device_id={"batch": partner_of(me, k)},
                    device_id_type=MESH,
                )
                flight[p].start()
            elif k == nb:
                flight[p] = pltpu.make_async_remote_copy(
                    src_ref=accs[nb - 1].at[p],
                    dst_ref=recv_x.at[p],
                    send_sem=x_send.at[p],
                    recv_sem=x_recv.at[p],
                    device_id={"rows": 1 - r},
                    device_id_type=MESH,
                )
                flight[p].start()
    last = accs[nb - 1]
    grad = jnp.concatenate([last[p, 0] + recv_x[p, 0] for p in range(pieces)], axis=1) / images
    grad_ref[...] = grad
    coef_ref[...] = jnp.zeros_like(coef_ref)
    ch = wc_ref.shape[1]
    kinds = kind_slices(ch, wp_ref.shape[1])
    nk = len(kinds)
    w_refs = (wc_ref, wp_ref)
    gain_refs = (gc_ref, gp_ref)
    first = 0
    for b, (which, col) in enumerate(kinds):
        count = w_refs[which].shape[0]
        piece = grad[first : first + count]
        first += count
        cent = w_refs[which][:, col : col + ch] - stat_ref[b : b + 1]
        s = jnp.sum(piece, axis=0, keepdims=True)
        off = piece - s / count
        src[b] = s
        src[nk + b] = jnp.sum(off * off, axis=0, keepdims=True)
        src[2 * nk + b] = jnp.sum(piece * cent, axis=0, keepdims=True)
    for copy in push_start(n, me, src, slots, s_send, s_recv):
        copy.wait()
    for b, (which, col) in enumerate(kinds):
        count = w_refs[which].shape[0]
        cols = slice(col, col + ch)
        fan = n * count
        _, gmean, gspread = merged(n, slots, b, nk + b, count, fan)
        at = 2 * nk + b
        proj = slots[0, at]
        for i in range(1, n):
            proj = proj + slots[i, at]
        mean = stat_ref[b : b + 1]
        spread = stat_ref[nk + b : nk + b + 1]
        factor = lax.rsqrt(spread + ws_eps)
        f2 = factor * factor
        one = gain_refs[which][cols][None] * factor
        two = one * f2 * proj
        grad_sq = one * one * jnp.maximum(gspread - f2 * proj * proj * (2.0 - f2 * spread), 0.0)
        weight_sq = spread + fan * (mean * mean)
        clip = jnp.minimum(1.0, clip_ratio * jnp.sqrt(weight_sq) * lax.rsqrt(grad_sq + norm_eps))
        coef_ref[b : b + 1] = clip * one
        coef_ref[nk + b : nk + b + 1] = gmean
        coef_ref[2 * nk + b : 2 * nk + b + 1] = clip * two


def update_kernel(grad_ref, coef_ref, stat_ref, wc_ref, wp_ref, mc_ref, mp_ref,
                  nwc_ref, nwp_ref, nmc_ref, nmp_ref):
    ch = wc_ref.shape[1]
    kinds = kind_slices(ch, wp_ref.shape[1])
    nk = len(kinds)
    first = 0
    for b, (which, col) in enumerate(kinds):
        w_ref = (wc_ref, wp_ref)[which]
        count = w_ref.shape[0]
        cols = slice(col, col + ch)
        w = w_ref[:, cols]
        grad = grad_ref[first : first + count]
        first += count
        clipped = coef_ref[b : b + 1] * (grad - coef_ref[nk + b : nk + b + 1]) - coef_ref[
            2 * nk + b : 2 * nk + b + 1
        ] * (w - stat_ref[b : b + 1])
        new_m = momentum_rate * (mc_ref, mp_ref)[which][:, cols] + clipped
        (nmc_ref, nmp_ref)[which][:, cols] = new_m
        (nwc_ref, nwp_ref)[which][:, cols] = w - learn_rate * (clipped + momentum_rate * new_m)


def shifted(vals, step, mc):
    rows = vals.shape[0]
    col = lax.broadcasted_iota(jnp.int32, vals.shape, 0)
    if step > 0:
        return jnp.where(col == mc - 1, 0.0, pltpu.roll(vals, rows - 1, 0))
    return jnp.where(col == 0, 0.0, pltpu.roll(vals, 1, 0))


def compute_kernel(n, order, mr, mc, gw, nc, np_, nblk,
                   x_ref, u_ref, hx_ref, hu_ref, full_ref,
                   ig_ref, part_ref,
                   kt, pt, xs, ys, hid, cg, pg):
    ch = x_ref.shape[1]
    groups = ch // gw
    wide = TAPS * gw
    px = mr * mc
    r = lax.axis_index("rows")
    for d in range(n):
        for p in range(ch // LANE):
            kt[d * nc : (d + 1) * nc, p * LANE : (p + 1) * LANE] = full_ref[p, order[d], :nc]
            for b in range(nblk):
                at = b * ch + p * LANE
                pt[d * np_ : (d + 1) * np_, at : at + LANE] = full_ref[
                    p, order[d], nc + b * np_ : nc + (b + 1) * np_
                ]

    def place(at, vals):
        act = gelu_parts(vals)[0].astype(BF16).astype(F32)
        for j in range(TAPS):
            moved = act if j == 1 else shifted(act, j - 1, mc)
            moved = moved.astype(BF16)
            for g in range(groups):
                xs[pl.ds(at, mc), g * wide + j * gw : g * wide + (j + 1) * gw] = moved[
                    :, g * gw : (g + 1) * gw
                ]

    for e in range(2):
        edge = hx_ref[e * mc : (e + 1) * mc].astype(F32)
        place(e * mc, jnp.where(r == 1, edge, 0.0))
        place((mr + 2 + e) * mc, jnp.where(r == 0, edge, 0.0))

    def body(row, carry):
        at = pl.multiple_of(row * mc, mc)
        place(pl.multiple_of(at + 2 * mc, mc), x_ref[pl.ds(at, mc)].astype(F32))
        return carry

    lax.fori_loop(0, mr, body, 0)

    def forward(e, up):
        hg = dot_nt(up, pt[...])
        for g in range(groups):
            acc = None
            for i in range(TAPS):
                term = dot_nn(
                    xs[pl.ds(pl.multiple_of((e + i) * mc, mc), up.shape[0]), g * wide : (g + 1) * wide],
                    kt[i * wide : (i + 1) * wide, g * gw : (g + 1) * gw],
                )
                acc = term if acc is None else acc + term
            h, slope = gelu_parts(acc)
            hid[pl.ds(pl.multiple_of(e * mc, mc), up.shape[0]), g * gw : (g + 1) * gw] = h.astype(BF16)
            grad = (hg[:, g * gw : (g + 1) * gw] * slope).astype(BF16).astype(F32)
            for q in range(up.shape[0] // mc):
                here = grad[q * mc : (q + 1) * mc]
                for j in range(TAPS):
                    moved = here if j == 1 else shifted(here, 1 - j, mc)
                    ys[pl.ds(pl.multiple_of((e + q) * mc, mc), mc), g * wide + j * gw : g * wide + (j + 1) * gw] = moved.astype(BF16)

    edge = hu_ref[...].astype(F32)
    forward(0, jnp.where(r == 1, edge, 0.0).astype(BF16))
    forward(mr + 1, jnp.where(r == 0, edge, 0.0).astype(BF16))
    many = 2 if mr % 2 == 0 else 1

    def fwd(t, carry):
        up = u_ref[pl.ds(pl.multiple_of(t * many * mc, mc), many * mc)]
        forward(1 + t * many, up)
        return carry

    lax.fori_loop(0, mr // many, fwd, 0)

    pg[...] = dot_tn(hid[mc : mc + px], u_ref[...])
    for g in range(groups):
        own = ys[mc : mc + px, g * wide + gw : g * wide + 2 * gw]
        for i in range(TAPS):
            cg[i * wide : (i + 1) * wide, g * gw : (g + 1) * gw] = dot_tn(
                xs[(1 + i) * mc : (1 + i) * mc + px, g * wide : (g + 1) * wide], own
            )
    for d in range(n):
        for p in range(ch // LANE):
            part_ref[p, order[d], :nc] = cg[
                d * nc : (d + 1) * nc, p * LANE : (p + 1) * LANE
            ].astype(BF16)
            for b in range(nblk):
                at = b * ch + p * LANE
                part_ref[p, order[d], nc + b * np_ : nc + (b + 1) * np_] = pg[
                    d * np_ : (d + 1) * np_, at : at + LANE
                ].astype(BF16)

    def back(t, carry):
        at = pl.multiple_of(t * many * mc, mc)
        for g in range(groups):
            acc = None
            for i in range(TAPS):
                for j in range(TAPS):
                    term = dot_nt(
                        ys[pl.ds(pl.multiple_of(at + (2 - i) * mc, mc), many * mc), g * wide + j * gw : g * wide + (j + 1) * gw],
                        kt[i * wide + j * gw : i * wide + (j + 1) * gw, g * gw : (g + 1) * gw],
                    )
                    acc = term if acc is None else acc + term
            slope = gelu_parts(x_ref[pl.ds(at, many * mc), g * gw : (g + 1) * gw].astype(F32))[1]
            ig_ref[pl.ds(at, many * mc), g * gw : (g + 1) * gw] = (acc * slope).astype(BF16)
        return carry

    lax.fori_loop(0, mr // many, back, 0)


def local(n, nrows, block_input, output_grad, conv_weight, conv_gain, conv_momentum,
          proj_weight, proj_gain, proj_momentum):
    assert nrows == 2
    nb = n.bit_length() - 1
    assert 2**nb == n
    _, mr, mc, ch = block_input.shape
    out = output_grad.shape[3]
    nc = conv_weight.shape[1]
    np_ = proj_weight.shape[1]
    nblk = out // ch
    gw = nc * n // (TAPS * TAPS)
    rows = nc + nblk * np_
    kinds = 1 + nblk
    pieces = ch // LANE
    order = [int(format(d, "0%db" % nb)[::-1], 2) for d in range(n)]
    px = mr * mc

    wc, wp, mc_, mp = conv_weight.T, proj_weight.T, conv_momentum.T, proj_momentum.T
    gc, gp = conv_gain, proj_gain
    x = block_input.reshape(px, ch)
    u = output_grad.reshape(px, out)
    vmem = pl.BlockSpec(memory_space=pltpu.VMEM)
    sdt = jax.ShapeDtypeStruct
    stat_rows = -(-2 * kinds // 8) * 8
    grad_rows = -(-3 * kinds // 8) * 8
    dma = pltpu.SemaphoreType.DMA
    full, stat, hx, hu = pl.pallas_call(
        functools.partial(gather_kernel, n, nb, pieces, 2 * mc, mc),
        out_shape=(
            sdt((pieces, n, rows, LANE), BF16),
            sdt((stat_rows, ch), F32),
            sdt((2 * mc, ch), BF16),
            sdt((mc, out), BF16),
        ),
        in_specs=[vmem] * 6,
        out_specs=(vmem,) * 4,
        scratch_shapes=[
            pltpu.VMEM((2 * kinds, 1, ch), F32),
            pltpu.VMEM((n, 2 * kinds, 1, ch), F32),
            dma((n - 1,)), dma((n - 1,)),
            dma((pieces, nb)), dma((pieces, nb)),
            dma((2,)), dma((2,)),
        ],
        compiler_params=pltpu.CompilerParams(collective_id=0, has_side_effects=True),
        name="gather",
    )(wc, wp, gc, gp, x, u)
    ig, part = pl.pallas_call(
        functools.partial(compute_kernel, n, order, mr, mc, gw, nc, np_, nblk),
        out_shape=(sdt((px, ch), BF16), sdt((pieces, n, rows, LANE), BF16)),
        in_specs=[vmem] * 5,
        out_specs=(vmem,) * 2,
        scratch_shapes=[
            pltpu.VMEM((n * nc, ch), BF16),
            pltpu.VMEM((n * np_, out), BF16),
            pltpu.VMEM(((mr + 4) * mc, TAPS * ch), BF16),
            pltpu.VMEM(((mr + 2) * mc, TAPS * ch), BF16),
            pltpu.VMEM(((mr + 2) * mc, ch), BF16),
            pltpu.VMEM((n * nc, ch), F32),
            pltpu.VMEM((n * np_, out), F32),
        ],
        name="compute",
    )(x, u, hx, hu, full)
    halves = [n >> (k + 1) for k in range(nb)]
    grad, coef = pl.pallas_call(
        functools.partial(reduce_kernel, n, nb, pieces, n),
        out_shape=(sdt((rows, ch), F32), sdt((grad_rows, ch), F32)),
        in_specs=[vmem] * 6,
        out_specs=(vmem,) * 2,
        scratch_shapes=[pltpu.VMEM((pieces, h, rows, LANE), BF16) for h in halves]
        + [pltpu.VMEM((pieces, h, rows, LANE), BF16 if h > 1 else F32) for h in halves]
        + [
            pltpu.VMEM((pieces, 1, rows, LANE), F32),
            pltpu.VMEM((3 * kinds, 1, ch), F32),
            pltpu.VMEM((n, 3 * kinds, 1, ch), F32),
            dma((pieces, nb)), dma((pieces, nb)),
            dma((n - 1,)), dma((n - 1,)),
            dma((pieces,)), dma((pieces,)),
        ],
        compiler_params=pltpu.CompilerParams(collective_id=1, has_side_effects=True),
        name="reduce",
    )(part, wc, wp, stat, gc, gp)
    nwc, nwp, nmc, nmp = pl.pallas_call(
        update_kernel,
        out_shape=(sdt((nc, ch), F32), sdt((np_, out), F32)) * 2,
        in_specs=[vmem] * 7,
        out_specs=(vmem,) * 4,
        name="update",
    )(grad, coef, stat, wc, wp, mc_, mp)
    return (ig.reshape(block_input.shape), nwc.T, nmc.T, nwp.T, nmp.T)


def solution(mesh):
    in_specs = (
        P("batch", "rows", None, None),
        P("batch", "rows", None, None),
        P(None, "batch"),
        P(),
        P(None, "batch"),
        P(None, "batch"),
        P(),
        P(None, "batch"),
    )
    out_specs = (
        P("batch", "rows", None, None),
        P(None, "batch"),
        P(None, "batch"),
        P(None, "batch"),
        P(None, "batch"),
    )
    body = functools.partial(local, mesh.shape["batch"], mesh.shape["rows"])
    return jax.shard_map(body, mesh=mesh, in_specs=in_specs, out_specs=out_specs, check_vma=False)
```
